512 devices in a mesh: grp: 2 (over y), ha: 16 (over z), ta: 8 (over x), cam: 2 (over core).
Axes of the slice: x: 8, y: 2, z: 16, core: 2. Of those that a mesh axis runs over, the one named last changes fastest.
The devices are a block of a 8x8x16 slice.
Arguments:
- video: bfloat16 [4, 32, 128, 48, 128], P(('grp', 'cam'), 'ta', 'ha'), parts along dimension 0, may hold values from -6 to 6
- norm1_gain: float32 [128], replicated, may hold values from 0.1 to 1.9
- norm1_shift: float32 [128], replicated, may hold values from -3 to 3
- conv1_weight: bfloat16 [3, 3, 3, 128, 128], replicated, may hold values from -0.109375 to 0.109375
- conv1_bias: float32 [128], replicated, may hold values from -3 to 3
- norm2_gain: float32 [128], replicated, may hold values from 0.1 to 1.9
- norm2_shift: float32 [128], replicated, may hold values from -3 to 3
- conv2_weight: bfloat16 [3, 3, 3, 128, 128], replicated, may hold values from -0.109375 to 0.109375
- conv2_bias: float32 [128], replicated, may hold values from -3 to 3
Outputs:
- encoded: bfloat16 [4, 32, 128, 48, 128], P(('grp', 'cam'), 'ta', 'ha'), parts along dimension 0
The draws below stay inside these ranges and needn't reach their ends.
There are 2 independent parts, one for each index of `grp`. The reference program is written for one: setup_inputs(seed, part) draws one part's arguments, and reference() takes and returns one part's arrays. A program takes and returns all parts, laid end to end along the dimension named above; an argument that names none is the same for every part. Nothing has to cross between parts.
All inputs are finite; a program needn't handle non-finite values.
Results may differ from the reference program's by a relative error of at most 0.0039.
Values may be sent and summed in bfloat16 or wider, within the bound.
No kernel may reach another device: no remote copies, remote signals or barrier semaphores. Data moves between devices by JAX's collectives and lax.ppermute only.
A program may use at most 128 MiB of HBM per device.

```python
import jax
import jax.numpy as jnp
from jax import lax

C = 128
WID = 48
CAMS = 2
FRAMES = 32
HEIGHT = 128


def steps_of(own_key, extent, pieces, smallest, largest):
    level, own = 1.0, jax.random.fold_in(own_key, 6)
    for dim, shards_of in pieces:
        steps = jnp.exp(jax.random.uniform(jax.random.fold_in(own, dim), (shards_of,), jnp.float32, smallest / len(pieces), largest / len(pieces)))
        level = level * jnp.repeat(steps, extent[dim] // shards_of).reshape([-1 if axis == dim else 1 for axis in range(len(extent))])
    return level


def noise(stream_key, dims, scale, reach, pieces=(), dtype=jnp.bfloat16):
    level = steps_of(stream_key, dims, pieces, -0.22, 0.18) if pieces else 1.0
    drawn = jax.random.normal(stream_key, dims, jnp.float32) * scale * level
    return jnp.minimum(jnp.maximum(drawn, -reach), reach).astype(dtype)


def setup_inputs(seed: int = 0, part: int = 0) -> dict:
    seeds = jax.random.split(jax.random.key(seed), 10)
    part_keys = jax.random.split(jax.random.fold_in(seeds[9], part), 10)
    return {
        "video": noise(part_keys[0], (CAMS, FRAMES, HEIGHT, WID, C), 1.0, 6.0, ((0, 2), (1, 8), (2, 16))),
        "norm1_gain": jnp.clip(1.0 + 0.18 * jax.random.normal(seeds[1], (C,), jnp.float32), 0.1, 1.9),
        "norm1_shift": noise(seeds[2], (C,), 0.5, 3.0, (), jnp.float32),
        "conv1_weight": noise(seeds[3], (3, 3, 3, C, C), (27 * C) ** -0.5, 0.109375),
        "conv1_bias": noise(seeds[4], (C,), 0.5, 3.0, (), jnp.float32),
        "norm2_gain": jnp.clip(1.0 + 0.18 * jax.random.normal(seeds[5], (C,), jnp.float32), 0.1, 1.9),
        "norm2_shift": noise(seeds[6], (C,), 0.5, 3.0, (), jnp.float32),
        "conv2_weight": noise(seeds[7], (3, 3, 3, C, C), (27 * C) ** -0.5, 0.109375),
        "conv2_bias": noise(seeds[8], (C,), 0.5, 3.0, (), jnp.float32),
    }


def activate(values, gain, shift):
    middle = lax.optimization_barrier(jnp.mean(values, axis=-1, keepdims=True))
    centred = values - middle
    spread = lax.optimization_barrier(jnp.mean(centred * centred, axis=-1, keepdims=True))
    normed = centred * lax.rsqrt(spread + 1e-06) * gain.astype(jnp.float32) + shift.astype(jnp.float32)
    return jax.nn.silu(normed)

def convolve(layer_input, weight, bias):
    leading = layer_input[:, :1]
    padded = jnp.concatenate([leading, leading, layer_input], axis=1)
    padded = jnp.pad(padded, ((0, 0), (0, 0), (1, 1), (1, 1), (0, 0)))
    result = lax.conv_general_dilated(padded.astype(jnp.float32), weight.astype(jnp.float32), (1, 1, 1), 'VALID', dimension_numbers=('NDHWC', 'DHWIO', 'NDHWC'), precision=lax.Precision.HIGHEST)
    return result + bias.astype(jnp.float32)

def reference(video, norm1_gain, norm1_shift, conv1_weight, conv1_bias, norm2_gain, norm2_shift, conv2_weight, conv2_bias):
    inputs = video.astype(jnp.float32)
    first_input = activate(inputs, norm1_gain, norm1_shift).astype(jnp.bfloat16)
    first_out = convolve(first_input, conv1_weight, conv1_bias)
    second_input = activate(first_out, norm2_gain, norm2_shift).astype(jnp.bfloat16)
    second_out = convolve(second_input, conv2_weight, conv2_bias)
    return (inputs + second_out).astype(jnp.bfloat16)
```

```python
import jax
import jax.numpy as jnp
from jax import lax
from jax.experimental import pallas as pl
from jax.experimental.pallas import tpu as pltpu
from jax.sharding import PartitionSpec as P

EPS = 1e-06


def activate(values, gain, shift):
    middle = jnp.mean(values, axis=-1, keepdims=True)
    centred = values - middle
    spread = jnp.mean(centred * centred, axis=-1, keepdims=True)
    normed = centred * lax.rsqrt(spread + EPS) * gain + shift
    return normed * (0.5 + 0.5 * jnp.tanh(0.5 * normed))


def put_shifted(ref, frame, pair, half, rows):
    width, channels = rows.shape
    column = lax.broadcasted_iota(jnp.int32, rows.shape, 0)
    before = jnp.where(column == 0, 0.0, pltpu.roll(rows, 1, 0))
    after = jnp.where(column == width - 1, 0.0, pltpu.roll(rows, width - 1, 0))
    lanes = pl.ds(half * channels, channels)
    ref[0, frame, pair, :, lanes] = before.astype(ref.dtype)
    ref[1, frame, pair, :, lanes] = rows.astype(ref.dtype)
    ref[2, frame, pair, :, lanes] = after.astype(ref.dtype)


def pair_taps(weight_ref, step_t, step_w):
    top, mid, low = (weight_ref[step_t, i, step_w] for i in range(3))
    none = jnp.zeros_like(top)
    upper = jnp.concatenate([jnp.concatenate([top, none], 1), jnp.concatenate([mid, top], 1)], 0)
    lower = jnp.concatenate([jnp.concatenate([low, mid], 1), jnp.concatenate([none, low], 1)], 0)
    return upper, lower


def conv_pairs(maps_ref, weight_ref, frames_of, pairs):
    width, lanes = maps_ref.shape[3:]
    total = None
    for step_w in range(3):
        for step_t in range(3):
            upper, lower = pair_taps(weight_ref, step_t, step_w)
            for rhs, skip in ((upper, 0), (lower, 1)):
                lhs = jnp.concatenate(
                    [maps_ref[step_w, f, skip : skip + pairs].reshape(pairs * width, lanes) for f in frames_of[step_t]], 0
                )
                part = jnp.dot(lhs, rhs, preferred_element_type=jnp.float32)
                total = part if total is None else total + part
    return total


def block_kernel(
    flags, video, behind, above, below, behind_above, behind_below,
    gain1, shift1, weight1, bias1, gain2, shift2, weight2, bias2, out, first, second,
):
    frames, rows, width, channels = video.shape
    is_start, has_above, has_below = flags[0] == 1, flags[1] == 1, flags[2] == 1
    inner = rows // 2

    def enter(ref, frame, row, to_frame, pair, valid):
        for half in range(2):
            values = activate(ref[frame, row + half].astype(jnp.float32), gain1[...], shift1[...])
            if valid is not None:
                values = jnp.where(valid, values, 0.0)
            put_shifted(first, to_frame, pair, half, values)

    def enter_frame(frame, carry):
        for ref, upper, lower, to in (
            (behind, behind_above, behind_below, frame),
            (video, above, below, frame + frames),
        ):
            enter(upper, frame, 0, to, 0, has_above)
            for k in range(inner):
                enter(ref, frame, 2 * k, to, k + 1, None)
            enter(lower, frame, 0, to, inner + 1, has_below)
        return carry

    lax.fori_loop(0, frames, enter_frame, 0)

    floor1 = jnp.where(is_start, frames, 0)
    floor2 = jnp.where(is_start, 2, 0)

    def layer1(step, carry):
        at = [2 * step, 2 * step + 1]
        frames_of = [[jnp.maximum(f + dt, floor1) for f in at] for dt in range(3)]
        total = conv_pairs(first, weight1, frames_of, inner + 1)
        total = total.reshape(2, inner + 1, width, 2 * channels)
        for i in range(2):
            for pair in range(inner + 1):
                for half in range(2):
                    values = total[i, pair, :, half * channels : (half + 1) * channels] + bias1[...]
                    values = activate(values, gain2[...], shift2[...])
                    if pair == 0 and half == 0:
                        values = jnp.where(has_above, values, 0.0)
                    if pair == inner and half == 1:
                        values = jnp.where(has_below, values, 0.0)
                    put_shifted(second, at[i], pair, half, values)
        return carry

    lax.fori_loop(0, (frames + 2) // 2, layer1, 0)

    def layer2(step, carry):
        at = [2 * step, 2 * step + 1]
        frames_of = [[jnp.maximum(f + dt, floor2) for f in at] for dt in range(3)]
        total = conv_pairs(second, weight2, frames_of, inner)
        total = total.reshape(2, inner, width, 2 * channels)
        for i in range(2):
            for pair in range(inner):
                for half in range(2):
                    values = total[i, pair, :, half * channels : (half + 1) * channels] + bias2[...]
                    row = 2 * pair + half
                    out[at[i], row] = (video[at[i], row].astype(jnp.float32) + values).astype(out.dtype)
        return carry

    lax.fori_loop(0, frames // 2, layer2, 0)


def body(
    video,
    norm1_gain,
    norm1_shift,
    conv1_weight,
    conv1_bias,
    norm2_gain,
    norm2_shift,
    conv2_weight,
    conv2_bias,
):
    clip = video[0]
    frames, rows, width, channels = clip.shape
    spans, slabs = lax.axis_size("ta"), lax.axis_size("ha")
    span, slab = lax.axis_index("ta"), lax.axis_index("ha")
    top, bottom = clip[:, :2], clip[:, rows - 2 :]

    def at(h, t):
        return h * spans + t

    behind = lax.ppermute(clip, "ta", [(t, t + 1) for t in range(spans - 1)])
    above = lax.ppermute(bottom, "ha", [(h, h + 1) for h in range(slabs - 1)])
    below = lax.ppermute(top, "ha", [(h + 1, h) for h in range(slabs - 1)])
    behind_above = lax.ppermute(
        bottom, ("ha", "ta"), [(at(h, t), at(h + 1, t + 1)) for h in range(slabs - 1) for t in range(spans - 1)]
    )
    behind_below = lax.ppermute(
        top, ("ha", "ta"), [(at(h + 1, t), at(h, t + 1)) for h in range(slabs - 1) for t in range(spans - 1)]
    )
    flags = jnp.stack([span == 0, slab > 0, slab < slabs - 1]).astype(jnp.int32)

    vmem = pl.BlockSpec(memory_space=pltpu.VMEM)
    vector = lambda v: v.reshape(1, channels)
    out = pl.pallas_call(
        block_kernel,
        out_shape=jax.ShapeDtypeStruct(clip.shape, clip.dtype),
        in_specs=[pl.BlockSpec(memory_space=pltpu.SMEM)] + [vmem] * 14,
        out_specs=vmem,
        scratch_shapes=[
            pltpu.VMEM((3, 2 * frames, rows // 2 + 2, width, 2 * channels), jnp.bfloat16),
            pltpu.VMEM((3, frames + 2, rows // 2 + 1, width, 2 * channels), jnp.bfloat16),
        ],
        compiler_params=pltpu.CompilerParams(vmem_limit_bytes=40 * 1024 * 1024),
        cost_estimate=pl.CostEstimate(flops=8 * 10**9, bytes_accessed=4 * 10**6, transcendentals=0),
        name="block",
    )(
        flags, clip, behind, above, below, behind_above, behind_below,
        vector(norm1_gain), vector(norm1_shift), conv1_weight, vector(conv1_bias),
        vector(norm2_gain), vector(norm2_shift), conv2_weight, vector(conv2_bias),
    )
    return out[None]


def solution(mesh):
    placed = (P(("grp", "cam"), "ta", "ha", None, None), P(), P(), P(), P(), P(), P(), P(), P())
    return jax.shard_map(
        body,
        mesh=mesh,
        in_specs=placed,
        out_specs=P(("grp", "cam"), "ta", "ha", None, None),
        check_vma=False,
    )
```

```python
import jax
import jax.numpy as jnp
from jax import lax
from jax.experimental import pallas as pl
from jax.experimental.pallas import tpu as pltpu
from jax.sharding import PartitionSpec as P


EPS = 1e-06
PAD = 8


def activate(values, gain, shift):
    middle = jnp.mean(values, axis=-1, keepdims=True)
    centred = values - middle
    spread = jnp.mean(centred * centred, axis=-1, keepdims=True)
    half = centred * lax.rsqrt(spread + EPS) * gain + shift
    return half + half * jnp.tanh(half)


def put_shifted(ref, frame, row, slot, values):
    width = values.shape[0]
    slot[PAD : PAD + width] = values
    ref[0, frame, row] = slot[PAD - 1 : PAD - 1 + width].astype(ref.dtype)
    ref[1, frame, row] = values.astype(ref.dtype)
    ref[2, frame, row] = slot[PAD + 1 : PAD + 1 + width].astype(ref.dtype)


def clear_slots(slots):
    for slot in range(slots.shape[0]):
        slots[slot, :PAD] = jnp.zeros((PAD, slots.shape[2]), slots.dtype)
        slots[slot, slots.shape[1] - PAD :] = jnp.zeros((PAD, slots.shape[2]), slots.dtype)


def pair_taps(weight_ref, step_t, step_w):
    top, mid, low = (weight_ref[step_t, i, step_w] for i in range(3))
    none = jnp.zeros_like(top)
    upper = jnp.concatenate([jnp.concatenate([top, none], 1), jnp.concatenate([mid, top], 1)], 0)
    lower = jnp.concatenate([jnp.concatenate([low, mid], 1), jnp.concatenate([none, low], 1)], 0)
    return upper, lower


def conv_pairs(maps_ref, weight_ref, taps, pairs):
    total = None
    for step_t, frame in taps:
        for step_w in range(3):
            for skip, rhs in enumerate(pair_taps(weight_ref, step_t, step_w)):
                rows = [2 * (skip + k) for k in range(pairs)]
                left = jnp.concatenate([maps_ref[step_w, frame, r] for r in rows], 0)
                right = jnp.concatenate([maps_ref[step_w, frame, r + 1] for r in rows], 0)
                lhs = jnp.concatenate([left, right], 1)
                part = jnp.dot(lhs, rhs, preferred_element_type=jnp.float32)
                total = part if total is None else total + part
    return total


def pick(total, row, width, channels):
    pair, half = divmod(row, 2)
    return total[pair * width : (pair + 1) * width, half * channels : (half + 1) * channels]


def ready_kernel(video, gain1, shift1, bias1, gain2, shift2, bias2, top, bottom, table, rows_in, sems):
    rows = video.shape[1]
    vectors = (gain1, shift1, bias1, gain2, shift2, bias2)
    loads = [
        pltpu.make_async_copy(video.at[:, :2], top, sems.at[0]),
        pltpu.make_async_copy(video.at[:, rows - 2 :], bottom, sems.at[1]),
    ] + [pltpu.make_async_copy(v, rows_in.at[i], sems.at[2 + i]) for i, v in enumerate(vectors)]
    for load in loads:
        load.start()
    for load in loads:
        load.wait()
    for i in range(len(vectors)):
        table[i] = rows_in[i] * (1.0 if i in (2, 5) else 0.5)


def near_kernel(
    flags, video, above, below, table, weight1_hbm, weight2_hbm,
    part1, part2, weight1, weight2, first, second, slots, sems,
):
    frames, rows, width, channels = video.shape
    loads = [
        pltpu.make_async_copy(weight1_hbm, weight1, sems.at[0]),
        pltpu.make_async_copy(weight2_hbm, weight2, sems.at[1]),
    ]
    for load in loads:
        load.start()
    clear_slots(slots)
    has_above, has_below = flags[1] == 1, flags[2] == 1
    g1, s1, b1, g2, s2, _ = (table[i] for i in range(6))

    def enter(frame):
        for row in range(-2, rows + 2):
            ref, at = (above, row + 2) if row < 0 else (below, row - rows) if row >= rows else (video, row)
            values = activate(ref[frame, at].astype(jnp.float32), g1, s1)
            if row < 0:
                values = jnp.where(has_above, values, 0.0)
            if row >= rows:
                values = jnp.where(has_below, values, 0.0)
            put_shifted(first, frame, row + 2, slots.at[frame * (rows + 4) + row + 2], values)

    def middle(total, to):
        for row in range(rows + 2):
            values = activate(pick(total, row, width, channels) + b1, g2, s2)
            if row == 0:
                values = jnp.where(has_above, values, 0.0)
            if row == rows + 1:
                values = jnp.where(has_below, values, 0.0)
            put_shifted(second, to, row, slots.at[(frames + to) * (rows + 4) + row], values)

    half = rows // 2
    enter(0)
    loads[0].wait()
    part1[0] = conv_pairs(first, weight1, [(2, 0)], half + 1)
    enter(1)
    part1[1] = conv_pairs(first, weight1, [(1, 0), (2, 1)], half + 1)
    enter(2)
    middle(conv_pairs(first, weight1, [(0, 0), (1, 1), (2, 2)], half + 1), 0)
    enter(3)
    middle(conv_pairs(first, weight1, [(0, 1), (1, 2), (2, 3)], half + 1), 1)
    loads[1].wait()
    part2[0] = conv_pairs(second, weight2, [(2, 0)], half)
    part2[1] = conv_pairs(second, weight2, [(1, 0), (2, 1)], half)


def far_kernel(
    flags, video, above, below, behind, behind_above, behind_below, part1, part2,
    table, weight1, weight2, out, first, second, slots,
):
    frames, rows, width, channels = video.shape
    clear_slots(slots)
    is_start, has_above, has_below = flags[0] == 1, flags[1] == 1, flags[2] == 1
    g1, s1, b1, g2, s2, b2 = (table[i] for i in range(6))

    def enter(frame):
        for row in range(-2, rows + 2):
            at = row + 2 if row < 0 else row - rows if row >= rows else row
            ref, own = (behind_above, above) if row < 0 else (behind_below, below) if row >= rows else (behind, video)
            values = ref[frame, at]
            if frame >= frames - 2:
                values = jnp.where(is_start, own[0, at], values)
            values = activate(values.astype(jnp.float32), g1, s1)
            if row < 0:
                values = jnp.where(has_above, values, 0.0)
            if row >= rows:
                values = jnp.where(has_below, values, 0.0)
            put_shifted(first, frame, row + 2, slots.at[frame * (rows + 4) + row + 2], values)

    def middle(total, to):
        for row in range(rows + 2):
            values = activate(pick(total, row, width, channels) + b1, g2, s2)
            if row == 0:
                values = jnp.where(has_above, values, 0.0)
            if row == rows + 1:
                values = jnp.where(has_below, values, 0.0)
            put_shifted(second, to, row, slots.at[(frames + to) * (rows + 4) + row], values)
            if to < 2:
                for step_w in range(3):
                    second[step_w, to, row] = jnp.where(is_start, second[step_w, 2, row], second[step_w, to, row])

    def leave(total, frame):
        for row in range(rows):
            values = pick(total, row, width, channels) + b2
            out[frame, row] = (video[frame, row].astype(jnp.float32) + values).astype(out.dtype)

    half = rows // 2
    enter(3)
    total = conv_pairs(first, weight1, [(0, 3)], half + 1) + part1[1]
    enter(2)
    middle(total, 3)
    total = conv_pairs(first, weight1, [(0, 2), (1, 3)], half + 1) + part1[0]
    enter(1)
    middle(total, 2)
    total = conv_pairs(first, weight1, [(0, 1), (1, 2), (2, 3)], half + 1)
    enter(0)
    middle(total, 1)
    total = conv_pairs(first, weight1, [(0, 0), (1, 1), (2, 2)], half + 1)
    leave(conv_pairs(second, weight2, [(0, 3)], half) + part2[1], 3)
    leave(conv_pairs(second, weight2, [(0, 2), (1, 3)], half) + part2[0], 2)
    middle(total, 0)
    leave(conv_pairs(second, weight2, [(0, 1), (1, 2), (2, 3)], half), 1)
    leave(conv_pairs(second, weight2, [(0, 0), (1, 1), (2, 2)], half), 0)


VMEM = pl.BlockSpec(memory_space=pltpu.VMEM)
SMEM = pl.BlockSpec(memory_space=pltpu.SMEM)
OUTSIDE = pl.BlockSpec(memory_space=pltpu.HBM)


def hbm(array):
    return pltpu.with_memory_space_constraint(array, pltpu.HBM)


def prepare(clip, *vectors):
    frames, _, width, channels = clip.shape
    edge = jax.ShapeDtypeStruct((frames, 2, width, channels), clip.dtype)
    return pl.pallas_call(
        ready_kernel,
        out_shape=[edge, edge, jax.ShapeDtypeStruct((6, 1, channels), jnp.float32)],
        in_specs=[OUTSIDE] * 7,
        out_specs=[VMEM] * 3,
        scratch_shapes=[pltpu.VMEM((6, 1, channels), jnp.float32), pltpu.SemaphoreType.DMA((8,))],
        compiler_params=pltpu.CompilerParams(vmem_limit_bytes=4 * 1024 * 1024),
        name="ready",
    )(hbm(clip), *(hbm(v.reshape(1, channels)) for v in vectors))


def local_block(flags, clip, behind, above, below, behind_above, behind_below, table, weight1, weight2):
    frames, rows, width, channels = clip.shape
    bf16, f32 = jnp.bfloat16, jnp.float32
    half = rows // 2
    maps = [
        pltpu.VMEM((3, frames, rows + 4, width, channels), bf16),
        pltpu.VMEM((3, frames, rows + 2, width, channels), bf16),
        pltpu.VMEM((2 * frames * (rows + 4), width + 2 * PAD, channels), f32),
    ]
    limit = pltpu.CompilerParams(vmem_limit_bytes=24 * 1024 * 1024)
    part1, part2, weight1, weight2 = pl.pallas_call(
        near_kernel,
        out_shape=[
            jax.ShapeDtypeStruct((2, (half + 1) * width, 2 * channels), f32),
            jax.ShapeDtypeStruct((2, half * width, 2 * channels), f32),
            jax.ShapeDtypeStruct(weight1.shape, bf16),
            jax.ShapeDtypeStruct(weight2.shape, bf16),
        ],
        in_specs=[SMEM] + [VMEM] * 4 + [OUTSIDE] * 2,
        out_specs=[VMEM] * 4,
        scratch_shapes=maps + [pltpu.SemaphoreType.DMA((2,))],
        compiler_params=limit,
        cost_estimate=pl.CostEstimate(flops=4 * 10**9, bytes_accessed=4 * 10**6, transcendentals=0),
        name="near",
    )(flags, clip, above, below, table, hbm(weight1), hbm(weight2))
    return pl.pallas_call(
        far_kernel,
        out_shape=jax.ShapeDtypeStruct(clip.shape, clip.dtype),
        in_specs=[SMEM] + [VMEM] * 11,
        out_specs=VMEM,
        scratch_shapes=maps,
        compiler_params=limit,
        cost_estimate=pl.CostEstimate(flops=4 * 10**9, bytes_accessed=4 * 10**6, transcendentals=0),
        name="far",
    )(
        flags, clip, above, below, behind, behind_above, behind_below, part1, part2,
        table, weight1, weight2,
    )


def body(
    video,
    norm1_gain,
    norm1_shift,
    conv1_weight,
    conv1_bias,
    norm2_gain,
    norm2_shift,
    conv2_weight,
    conv2_bias,
):
    clip = video[0]
    spans, slabs = lax.axis_size("ta"), lax.axis_size("ha")
    span, slab = lax.axis_index("ta"), lax.axis_index("ha")

    def at(h, t):
        return h * spans + t

    up = [(h, h + 1) for h in range(slabs - 1)]
    on = [(t, t + 1) for t in range(spans - 1)]

    behind = lax.ppermute(clip, "ta", on)
    top, bottom, table = prepare(clip, norm1_gain, norm1_shift, conv1_bias, norm2_gain, norm2_shift, conv2_bias)
    behind_below = lax.ppermute(top, ("ha", "ta"), [(at(h, t), at(g, n)) for g, h in up for t, n in on])
    above = lax.ppermute(bottom, "ha", up)
    behind_above = lax.ppermute(bottom, ("ha", "ta"), [(at(g, t), at(h, n)) for g, h in up for t, n in on])
    below = lax.ppermute(top, "ha", [(h, g) for g, h in up])
    flags = jnp.stack([span == 0, slab > 0, slab < slabs - 1]).astype(jnp.int32)
    out = local_block(flags, clip, behind, above, below, behind_above, behind_below, table, conv1_weight, conv2_weight)
    return out[None]


def solution(mesh):
    placed = (P(("grp", "cam"), "ta", "ha", None, None), P(), P(), P(), P(), P(), P(), P(), P())
    return jax.shard_map(
        body,
        mesh=mesh,
        in_specs=placed,
        out_specs=P(("grp", "cam"), "ta", "ha", None, None),
        check_vma=False,
    )
```

```python
import functools

import jax
import jax.numpy as jnp
from jax import lax
from jax.experimental import pallas as pl
from jax.experimental.pallas import tpu as pltpu
from jax.sharding import PartitionSpec as P


EPS = 1e-06
PAD = 8


def activate(values, gain, shift):
    middle = jnp.mean(values, axis=-1, keepdims=True)
    centred = values - middle
    spread = jnp.mean(centred * centred, axis=-1, keepdims=True)
    half = centred * lax.rsqrt(spread + EPS) * gain + shift
    return half + half * jnp.tanh(half)


def put_shifted(ref, frame, row, slot, values):
    width = values.shape[0]
    slot[PAD : PAD + width] = values
    ref[0, frame, row] = slot[PAD - 1 : PAD - 1 + width].astype(ref.dtype)
    ref[1, frame, row] = values.astype(ref.dtype)
    ref[2, frame, row] = slot[PAD + 1 : PAD + 1 + width].astype(ref.dtype)


def clear_slots(slots):
    for slot in range(slots.shape[0]):
        slots[slot, :PAD] = jnp.zeros((PAD, slots.shape[2]), slots.dtype)
        slots[slot, slots.shape[1] - PAD :] = jnp.zeros((PAD, slots.shape[2]), slots.dtype)


def pair_taps(weight_ref, step_t, step_w):
    top, mid, low = (weight_ref[step_t, i, step_w] for i in range(3))
    none = jnp.zeros_like(top)
    upper = jnp.concatenate([jnp.concatenate([top, none], 1), jnp.concatenate([mid, top], 1)], 0)
    lower = jnp.concatenate([jnp.concatenate([low, mid], 1), jnp.concatenate([none, low], 1)], 0)
    return upper, lower


def conv_pairs(maps_ref, weight_ref, taps, pairs):
    total = None
    for step_t, frame in taps:
        for step_w in range(3):
            for skip, rhs in enumerate(pair_taps(weight_ref, step_t, step_w)):
                rows = [2 * (skip + k) for k in range(pairs)]
                left = jnp.concatenate([maps_ref[step_w, frame, r] for r in rows], 0)
                right = jnp.concatenate([maps_ref[step_w, frame, r + 1] for r in rows], 0)
                lhs = jnp.concatenate([left, right], 1)
                part = jnp.dot(lhs, rhs, preferred_element_type=jnp.float32)
                total = part if total is None else total + part
    return total


def pick(total, row, width, channels):
    pair, half = divmod(row, 2)
    return total[pair * width : (pair + 1) * width, half * channels : (half + 1) * channels]


def ready_kernel(video, top, bottom):
    top[...] = video[:, : top.shape[1]]
    bottom[...] = video[:, video.shape[1] - bottom.shape[1] :]


def masked(values, valid):
    return values if valid is None else jnp.where(valid, values, 0.0)


def own_sums(video, vectors, weights_hbm, table, weights, part1, second, first, slots, sems):
    frames, rows, width, channels = video.shape
    loads = [pltpu.make_async_copy(v, table.at[i], sems.at[i]) for i, v in enumerate(vectors)]
    loads += [pltpu.make_async_copy(h, w, sems.at[6 + i]) for i, (h, w) in enumerate(zip(weights_hbm, weights))]
    for load in loads:
        load.start()
    clear_slots(slots)
    for load in loads[:6]:
        load.wait()
    g1, s1, b1, g2, s2, _ = (table[i] for i in range(6))
    g1, s1, g2, s2 = 0.5 * g1, 0.5 * s1, 0.5 * g2, 0.5 * s2
    half = rows // 2

    def enter(frame):
        for row in range(rows):
            values = activate(video[frame, row].astype(jnp.float32), g1, s1)
            put_shifted(first, frame, row + 2, slots.at[frame * rows + row], values)
        for row in (0, 1, rows + 2, rows + 3):
            for step_w in range(3):
                first[step_w, frame, row] = jnp.zeros((width, channels), first.dtype)

    def middle(total, frame, to):
        part1[frame] = total
        for row in range(2, rows):
            values = activate(pick(total, row, width, channels) + b1, g2, s2)
            put_shifted(second, to, row, slots.at[(frames + to) * rows + row], values)

    enter(0)
    loads[6].wait()
    part1[0] = conv_pairs(first, weights[0], [(2, 0)], half + 1)
    enter(1)
    part1[1] = conv_pairs(first, weights[0], [(1, 0), (2, 1)], half + 1)
    enter(2)
    middle(conv_pairs(first, weights[0], [(0, 0), (1, 1), (2, 2)], half + 1), 2, 0)
    enter(3)
    middle(conv_pairs(first, weights[0], [(0, 1), (1, 2), (2, 3)], half + 1), 3, 1)
    loads[7].wait()


def near_kernel(
    place, video, v0, v1, v2, v3, v4, v5, weight1_hbm, weight2_hbm,
    part1, second, table, weight1, weight2, first, slots, sems,
):
    is_top = jnp.logical_not(place()[1])

    @pl.when(jnp.logical_not(is_top))
    def _():
        own_sums(
            video, (v0, v1, v2, v3, v4, v5), (weight1_hbm, weight2_hbm),
            table, (weight1, weight2), part1, second, first, slots, sems,
        )


def edge_kernel(
    place, video, above, below, v0, v1, v2, v3, v4, v5, weight1_hbm, weight2_hbm, *refs,
):
    part1, second, table, weight1, weight2, part2, first, halo, slots, sems = refs[5:]
    frames, rows, width, channels = video.shape
    _, has_above, has_below = place()

    @pl.when(jnp.logical_not(has_above))
    def _():
        own_sums(
            video, (v0, v1, v2, v3, v4, v5), (weight1_hbm, weight2_hbm),
            table, (weight1, weight2), part1, second, first, slots, sems,
        )

    clear_slots(slots)
    g1, s1, b1, g2, s2, _ = (table[i] for i in range(6))
    g1, s1, g2, s2 = 0.5 * g1, 0.5 * s1, 0.5 * g2, 0.5 * s2
    half = rows // 2
    sides = ((above, has_above, 0, 0), (below, has_below, 1, half))
    for frame in range(frames):
        for ref, valid, side, _ in sides:
            for k in range(2):
                values = masked(activate(ref[frame, k].astype(jnp.float32), g1, s1), valid)
                put_shifted(halo, frame, 2 * side + k, slots.at[4 * frame + 2 * side + k], values)
    sums = {}
    for _, _, side, pair in sides:
        for step_t in range(3):
            count = frames - 2 + step_t
            total = None
            for step_w in range(3):
                rhs = pair_taps(weight1, step_t, step_w)[side]
                left = jnp.concatenate([halo[step_w, f, 2 * side] for f in range(count)], 0)
                right = jnp.concatenate([halo[step_w, f, 2 * side + 1] for f in range(count)], 0)
                part = jnp.dot(jnp.concatenate([left, right], 1), rhs, preferred_element_type=jnp.float32)
                total = part if total is None else total + part
            for f in range(count):
                to = f + 2 - step_t
                part = total[f * width : (f + 1) * width]
                sums[side, to] = part if (side, to) not in sums else sums[side, to] + part
    for to in range(frames):
        for _, valid, side, pair in sides:
            total = part1[to, pair * width : (pair + 1) * width] + sums[side, to]
            if to < 2:
                part1[to, pair * width : (pair + 1) * width] = total
                continue
            for k in range(2):
                row = 2 * pair + k
                values = activate(pick(total, k, width, channels) + b1, g2, s2)
                values = masked(values, valid if row in (0, rows + 1) else None)
                put_shifted(second, to - 2, row, slots.at[4 * (frames + to) + 2 * side + k], values)
    part2[0] = conv_pairs(second, weight2, [(2, 0)], half)
    part2[1] = conv_pairs(second, weight2, [(1, 0), (2, 1)], half)


def far_kernel(
    place, video, above, below, behind, behind_above, behind_below, part1, part2,
    table, weight1, weight2, out, first, second, slots, held, sems,
):
    frames, rows, width, channels = video.shape
    clear_slots(slots)
    is_start, has_above, has_below = place()
    g1, s1, b1, g2, s2, b2 = (table[i] for i in range(6))
    g1, s1, g2, s2 = 0.5 * g1, 0.5 * s1, 0.5 * g2, 0.5 * s2

    def enter(frame):
        for row in range(-2, rows + 2):
            at = row + 2 if row < 0 else row - rows if row >= rows else row
            ref, own = (behind_above, above) if row < 0 else (behind_below, below) if row >= rows else (behind, video)
            values = ref[frame, at]
            if frame >= frames - 2:
                values = jnp.where(is_start, own[0, at], values)
            values = activate(values.astype(jnp.float32), g1, s1)
            values = masked(values, has_above if row < 0 else has_below if row >= rows else None)
            put_shifted(first, frame, row + 2, slots.at[frame * (rows + 4) + row + 2], values)

    def middle(total, to):
        for row in range(rows + 2):
            values = activate(pick(total, row, width, channels) + b1, g2, s2)
            values = masked(values, has_above if row == 0 else has_below if row == rows + 1 else None)
            if to < 2:
                values = jnp.where(is_start, slots[(frames + 2) * (rows + 4) + row, PAD : PAD + width], values)
            put_shifted(second, to, row, slots.at[(frames + to) * (rows + 4) + row], values)

    def leave(total, frame):
        for row in range(rows):
            values = pick(total, row, width, channels) + b2
            held[frame, row] = (video[frame, row].astype(jnp.float32) + values).astype(out.dtype)
        pltpu.make_async_copy(held.at[frame], out.at[frame], sems.at[frame]).start()

    half = rows // 2
    enter(3)
    total = conv_pairs(first, weight1, [(0, 3)], half + 1) + part1[1]
    enter(2)
    middle(total, 3)
    total = conv_pairs(first, weight1, [(0, 2), (1, 3)], half + 1) + part1[0]
    enter(1)
    middle(total, 2)
    total = conv_pairs(first, weight1, [(0, 1), (1, 2), (2, 3)], half + 1)
    enter(0)
    middle(total, 1)
    total = conv_pairs(first, weight1, [(0, 0), (1, 1), (2, 2)], half + 1)
    leave(conv_pairs(second, weight2, [(0, 3)], half) + part2[1], 3)
    leave(conv_pairs(second, weight2, [(0, 2), (1, 3)], half) + part2[0], 2)
    middle(total, 0)
    leave(conv_pairs(second, weight2, [(0, 1), (1, 2), (2, 3)], half), 1)
    leave(conv_pairs(second, weight2, [(0, 0), (1, 1), (2, 2)], half), 0)
    for frame in range(frames):
        pltpu.make_async_copy(held.at[frame], out.at[frame], sems.at[frame]).wait()


VMEM = pl.BlockSpec(memory_space=pltpu.VMEM)
OUTSIDE = pl.BlockSpec(memory_space=pltpu.HBM)
MIB = 1024 * 1024


def hbm(array):
    return pltpu.with_memory_space_constraint(array, pltpu.HBM)


def cost(flops):
    return pl.CostEstimate(flops=flops, bytes_accessed=4 * 10**6, transcendentals=0)


def ready(clip):
    frames, _, width, channels = clip.shape
    edge = jax.ShapeDtypeStruct((frames, 2, width, channels), clip.dtype)
    return pl.pallas_call(
        ready_kernel,
        out_shape=[edge, edge],
        in_specs=[VMEM],
        out_specs=[VMEM] * 2,
        compiler_params=pltpu.CompilerParams(vmem_limit_bytes=4 * MIB),
        name="ready",
    )(clip)


def near(place, clip, vectors, weight1, weight2):
    frames, rows, width, channels = clip.shape
    bf16, f32 = jnp.bfloat16, jnp.float32
    outside = [hbm(v.reshape(1, channels)) for v in vectors] + [hbm(weight1), hbm(weight2)]
    return pl.pallas_call(
        functools.partial(near_kernel, place),
        out_shape=[
            jax.ShapeDtypeStruct((frames, (rows // 2 + 1) * width, 2 * channels), f32),
            jax.ShapeDtypeStruct((3, 2, rows + 2, width, channels), bf16),
            jax.ShapeDtypeStruct((6, 1, channels), f32),
            jax.ShapeDtypeStruct(weight1.shape, bf16),
            jax.ShapeDtypeStruct(weight2.shape, bf16),
        ],
        in_specs=[VMEM] + [OUTSIDE] * 8,
        out_specs=[VMEM] * 5,
        scratch_shapes=[
            pltpu.VMEM((3, frames, rows + 4, width, channels), bf16),
            pltpu.VMEM(((frames + 2) * rows, width + 2 * PAD, channels), f32),
            pltpu.SemaphoreType.DMA((8,)),
        ],
        compiler_params=pltpu.CompilerParams(vmem_limit_bytes=24 * MIB),
        cost_estimate=cost(4 * 10**9),
        name="near",
    )(clip, *outside)


def edge(place, clip, above, below, vectors, weight1, weight2, made):
    frames, rows, width, channels = clip.shape
    bf16, f32 = jnp.bfloat16, jnp.float32
    outside = [hbm(v.reshape(1, channels)) for v in vectors] + [hbm(weight1), hbm(weight2)]
    return pl.pallas_call(
        functools.partial(edge_kernel, place),
        out_shape=[jax.ShapeDtypeStruct(m.shape, m.dtype) for m in made]
        + [jax.ShapeDtypeStruct((2, rows // 2 * width, 2 * channels), f32)],
        in_specs=[VMEM] * 3 + [OUTSIDE] * 8 + [VMEM] * 5,
        out_specs=[VMEM] * 6,
        input_output_aliases={11 + i: i for i in range(5)},
        scratch_shapes=[
            pltpu.VMEM((3, frames, rows + 4, width, channels), bf16),
            pltpu.VMEM((3, frames, 4, width, channels), bf16),
            pltpu.VMEM(((frames + 2) * rows, width + 2 * PAD, channels), f32),
            pltpu.SemaphoreType.DMA((8,)),
        ],
        compiler_params=pltpu.CompilerParams(vmem_limit_bytes=24 * MIB),
        cost_estimate=cost(2 * 10**9),
        name="edge",
    )(clip, above, below, *outside, *made)


def far(place, clip, above, below, behind, behind_above, behind_below, part1, part2, table, weight1, weight2):
    frames, rows, width, channels = clip.shape
    bf16, f32 = jnp.bfloat16, jnp.float32
    return pl.pallas_call(
        functools.partial(far_kernel, place),
        out_shape=jax.ShapeDtypeStruct(clip.shape, clip.dtype),
        in_specs=[VMEM] * 11,
        out_specs=OUTSIDE,
        scratch_shapes=[
            pltpu.VMEM((3, frames, rows + 4, width, channels), bf16),
            pltpu.VMEM((3, frames, rows + 2, width, channels), bf16),
            pltpu.VMEM((2 * frames * (rows + 4), width + 2 * PAD, channels), f32),
            pltpu.VMEM(clip.shape, clip.dtype),
            pltpu.SemaphoreType.DMA((frames,)),
        ],
        compiler_params=pltpu.CompilerParams(vmem_limit_bytes=24 * MIB),
        cost_estimate=cost(4 * 10**9),
        name="far",
    )(clip, above, below, behind, behind_above, behind_below, part1, part2, table, weight1, weight2)


def body(
    video,
    norm1_gain,
    norm1_shift,
    conv1_weight,
    conv1_bias,
    norm2_gain,
    norm2_shift,
    conv2_weight,
    conv2_bias,
):
    clip = video[0]
    spans, slabs = lax.axis_size("ta"), lax.axis_size("ha")
    vectors = (norm1_gain, norm1_shift, conv1_bias, norm2_gain, norm2_shift, conv2_bias)

    def place():
        slab = lax.axis_index("ha")
        return lax.axis_index("ta") == 0, slab > 0, slab < slabs - 1

    def at(h, t):
        return h * spans + t

    up = [(h, h + 1) for h in range(slabs - 1)]
    on = [(t, t + 1) for t in range(spans - 1)]

    behind = lax.ppermute(clip, "ta", on)
    top, bottom = ready(clip)
    behind_below = lax.ppermute(top, ("ha", "ta"), [(at(h, t), at(g, n)) for g, h in up for t, n in on])
    above = lax.ppermute(bottom, "ha", up)
    made = near(place, clip, vectors, conv1_weight, conv2_weight)
    below = lax.ppermute(top, "ha", [(h, g) for g, h in up])
    behind_above = lax.ppermute(bottom, ("ha", "ta"), [(at(g, t), at(h, n)) for g, h in up for t, n in on])
    *made, part2 = edge(place, clip, above, below, vectors, conv1_weight, conv2_weight, made)
    part1, _, table, weight1, weight2 = made
    out = far(
        place, clip, above, below, behind, behind_above, behind_below, part1, part2, table, weight1, weight2
    )
    return out[None]


def solution(mesh):
    placed = (P(("grp", "cam"), "ta", "ha", None, None), P(), P(), P(), P(), P(), P(), P(), P())
    return jax.shard_map(
        body,
        mesh=mesh,
        in_specs=placed,
        out_specs=P(("grp", "cam"), "ta", "ha", None, None),
        check_vma=False,
    )
```

```python
import functools

import jax
import jax.numpy as jnp
from jax import lax
from jax.experimental import pallas as pl
from jax.experimental.pallas import tpu as pltpu
from jax.sharding import PartitionSpec as P


EPS = 1e-06
PAD = 8


def activate(values, gain, shift):
    middle = jnp.mean(values, axis=-1, keepdims=True)
    centred = values - middle
    spread = jnp.mean(centred * centred, axis=-1, keepdims=True)
    half = centred * lax.rsqrt(spread + EPS) * gain + shift
    return half + half * jnp.tanh(half)


def put_shifted(ref, frame, row, slots, group, values):
    width = values.shape[0]
    start = row * (width + PAD) + PAD
    slots[group, start : start + width] = values
    ref[0, frame, row] = slots[group, start - 1 : start - 1 + width].astype(ref.dtype)
    ref[1, frame, row] = values.astype(ref.dtype)
    ref[2, frame, row] = slots[group, start + 1 : start + 1 + width].astype(ref.dtype)


def slot_shape(groups, rows, width, channels):
    return groups, rows * (width + PAD) + PAD, channels


def clear_slots(slots, width):
    for group in range(slots.shape[0]):
        for start in range(0, slots.shape[1], width + PAD):
            slots[group, start : start + PAD] = jnp.zeros((PAD, slots.shape[2]), slots.dtype)


def pair_taps(weight_ref, step_t, step_w):
    top, mid, low = (weight_ref[step_t, i, step_w] for i in range(3))
    none = jnp.zeros_like(top)
    upper = jnp.concatenate([jnp.concatenate([top, none], 1), jnp.concatenate([mid, top], 1)], 0)
    lower = jnp.concatenate([jnp.concatenate([low, mid], 1), jnp.concatenate([none, low], 1)], 0)
    return upper, lower


def conv_pairs(maps_ref, weight_ref, taps, pairs):
    total = None
    for step_t, frame in taps:
        for step_w in range(3):
            for skip, rhs in enumerate(pair_taps(weight_ref, step_t, step_w)):
                rows = [2 * (skip + k) for k in range(pairs)]
                left = jnp.concatenate([maps_ref[step_w, frame, r] for r in rows], 0)
                right = jnp.concatenate([maps_ref[step_w, frame, r + 1] for r in rows], 0)
                lhs = jnp.concatenate([left, right], 1)
                part = jnp.dot(lhs, rhs, preferred_element_type=jnp.float32)
                total = part if total is None else total + part
    return total


def pick(total, row, width, channels):
    pair, half = divmod(row, 2)
    return total[pair * width : (pair + 1) * width, half * channels : (half + 1) * channels]


def ready_kernel(video, top, bottom):
    top[...] = video[:, : top.shape[1]]
    bottom[...] = video[:, video.shape[1] - bottom.shape[1] :]


def masked(values, valid):
    return values if valid is None else jnp.where(valid, values, 0.0)


def own_sums(video, vectors, weights_hbm, table, weights, part1, second, first, slots, sems):
    _, rows, width, channels = video.shape
    loads = [pltpu.make_async_copy(v, table.at[i], sems.at[i]) for i, v in enumerate(vectors)]
    loads += [pltpu.make_async_copy(h, w, sems.at[6 + i]) for i, (h, w) in enumerate(zip(weights_hbm, weights))]
    for load in loads:
        load.start()
    clear_slots(slots, width)
    for load in loads[:6]:
        load.wait()
    g1, s1, b1, g2, s2, _ = (table[i] for i in range(6))
    g1, s1, g2, s2 = 0.5 * g1, 0.5 * s1, 0.5 * g2, 0.5 * s2
    half = rows // 2

    def enter(frame):
        for row in range(rows):
            values = activate(video[frame, row].astype(jnp.float32), g1, s1)
            put_shifted(first, frame, row + 2, slots, frame % 2, values)
        for row in (0, 1, rows + 2, rows + 3):
            for step_w in range(3):
                first[step_w, frame, row] = jnp.zeros((width, channels), first.dtype)

    def middle(total, frame, to):
        part1[frame] = total
        for row in range(2, rows):
            values = activate(pick(total, row, width, channels) + b1, g2, s2)
            put_shifted(second, to, row, slots, 2 + to, values)

    enter(0)
    loads[6].wait()
    part1[0] = conv_pairs(first, weights[0], [(2, 0)], half + 1)
    enter(1)
    part1[1] = conv_pairs(first, weights[0], [(1, 0), (2, 1)], half + 1)
    enter(2)
    middle(conv_pairs(first, weights[0], [(0, 0), (1, 1), (2, 2)], half + 1), 2, 0)
    enter(3)
    middle(conv_pairs(first, weights[0], [(0, 1), (1, 2), (2, 3)], half + 1), 3, 1)
    loads[7].wait()


def near_kernel(
    place, video, v0, v1, v2, v3, v4, v5, weight1_hbm, weight2_hbm,
    part1, second, table, weight1, weight2, first, slots, sems,
):
    is_top = jnp.logical_not(place()[1])

    @pl.when(jnp.logical_not(is_top))
    def _():
        own_sums(
            video, (v0, v1, v2, v3, v4, v5), (weight1_hbm, weight2_hbm),
            table, (weight1, weight2), part1, second, first, slots, sems,
        )


def edge_kernel(
    place, video, above, below, v0, v1, v2, v3, v4, v5, weight1_hbm, weight2_hbm, *refs,
):
    part1, second, table, weight1, weight2, first, halo, slots, sems = refs[5:]
    frames, rows, width, channels = video.shape
    _, has_above, has_below = place()

    @pl.when(jnp.logical_not(has_above))
    def _():
        own_sums(
            video, (v0, v1, v2, v3, v4, v5), (weight1_hbm, weight2_hbm),
            table, (weight1, weight2), part1, second, first, slots, sems,
        )

    clear_slots(slots, width)
    g1, s1, b1, g2, s2, _ = (table[i] for i in range(6))
    g1, s1, g2, s2 = 0.5 * g1, 0.5 * s1, 0.5 * g2, 0.5 * s2
    half = rows // 2
    sides = ((above, has_above, 0, 0), (below, has_below, 1, half))
    for frame in range(frames):
        for ref, valid, side, _ in sides:
            for k in range(2):
                values = masked(activate(ref[frame, k].astype(jnp.float32), g1, s1), valid)
                put_shifted(halo, frame, 2 * side + k, slots, frame, values)
    sums = {}
    for _, _, side, pair in sides:
        for step_t in range(3):
            count = frames - 2 + step_t
            total = None
            for step_w in range(3):
                rhs = pair_taps(weight1, step_t, step_w)[side]
                left = jnp.concatenate([halo[step_w, f, 2 * side] for f in range(count)], 0)
                right = jnp.concatenate([halo[step_w, f, 2 * side + 1] for f in range(count)], 0)
                part = jnp.dot(jnp.concatenate([left, right], 1), rhs, preferred_element_type=jnp.float32)
                total = part if total is None else total + part
            for f in range(count):
                to = f + 2 - step_t
                part = total[f * width : (f + 1) * width]
                sums[side, to] = part if (side, to) not in sums else sums[side, to] + part
    for to in range(frames):
        for _, valid, side, pair in sides:
            total = part1[to, pair * width : (pair + 1) * width] + sums[side, to]
            if to < 2:
                part1[to, pair * width : (pair + 1) * width] = total
                continue
            for k in range(2):
                row = 2 * pair + k
                values = activate(pick(total, k, width, channels) + b1, g2, s2)
                values = masked(values, valid if row in (0, rows + 1) else None)
                put_shifted(second, to - 2, row, slots, to - 2, values)


def conv_same(maps_ref, weight_ref, taps, rows):
    total = None
    for step_t, frame in taps:
        for step_w in range(3):
            top, mid, low = (weight_ref[step_t, i, step_w] for i in range(3))
            rhs = jnp.concatenate([jnp.concatenate([mid, top], 1), jnp.concatenate([low, mid], 1)], 0)
            left = jnp.concatenate([maps_ref[step_w, frame, r + 1] for r in rows], 0)
            right = jnp.concatenate([maps_ref[step_w, frame, r + 2] for r in rows], 0)
            part = jnp.dot(jnp.concatenate([left, right], 1), rhs, preferred_element_type=jnp.float32)
            total = part if total is None else total + part
    return total


def conv_next(maps_ref, weight_ref, pairs, rows, step_h):
    total = None
    for frames, steps in pairs:
        for step_w in range(3):
            none = jnp.zeros(weight_ref.shape[3:], weight_ref.dtype)
            blocks = [[none if t is None else weight_ref[t, step_h, step_w] for t in line] for line in steps]
            rhs = jnp.concatenate([jnp.concatenate(line, 1) for line in blocks], 0)
            sides = [jnp.concatenate([maps_ref[step_w, f, r + 3 * (step_h // 2)] for r in rows], 0) for f in frames]
            part = jnp.dot(jnp.concatenate(sides, 1), rhs, preferred_element_type=jnp.float32)
            total = part if total is None else total + part
    return total


def far_kernel(
    place, video, above, below, behind, behind_above, behind_below, part1, own,
    table, weight1, weight2, out, first, second, slots, held, sems,
):
    frames, rows, width, channels = video.shape
    is_start, has_above, has_below = place()
    g1, s1, b1, g2, s2, b2 = (table[i] for i in range(6))
    g1, s1, g2, s2 = 0.5 * g1, 0.5 * s1, 0.5 * g2, 0.5 * s2
    clear_slots(slots, width)

    def enter(frame):
        for row in range(-2, rows + 2):
            at = row + 2 if row < 0 else row - rows if row >= rows else row
            ref, mine = (behind_above, above) if row < 0 else (behind_below, below) if row >= rows else (behind, video)
            values = ref[frame, at]
            if frame >= frames - 2:
                values = jnp.where(is_start, mine[0, at], values)
            values = activate(values.astype(jnp.float32), g1, s1)
            values = masked(values, has_above if row < 0 else has_below if row >= rows else None)
            put_shifted(first, frame, row + 2, slots, frame % 2, values)

    def gather(same, sides, which, more, row):
        pair, half = divmod(row, 2)
        lines = slice(pair * width, (pair + 1) * width)
        values = same[lines, half * channels : (half + 1) * channels]
        values = values + sides[half][lines, which * channels : (which + 1) * channels]
        return values if more is None else values + more[lines, half * channels : (half + 1) * channels]

    def middle(to, same, sides, which, more, group):
        for row in range(rows + 2):
            values = activate(gather(same, sides, which, more, row) + b1, g2, s2)
            values = masked(values, has_above if row == 0 else has_below if row == rows + 1 else None)
            if to < 2:
                start = row * (width + PAD) + PAD
                values = jnp.where(is_start, slots[3, start : start + width], values)
            put_shifted(second, to, row, slots, group, values)

    def leave(frame, same, sides, which, more):
        for row in range(rows):
            values = gather(same, sides, which, more, row) + b2
            held[frame, row] = (video[frame, row].astype(jnp.float32) + values).astype(out.dtype)
        pltpu.make_async_copy(held.at[frame], out.at[frame], sems.at[frame]).start()

    half = rows // 2
    ins, outs = range(0, rows + 2, 2), range(0, rows, 2)
    early, late = (((0, 1), ((0, None), (1, 0))), ((2, 3), ((2, 1), (None, 2))))
    last = ((2, 3), ((0, None), (1, 0)))
    own3 = conv_pairs(own, weight2, [(1, 0), (2, 1)], half)
    own2 = conv_pairs(own, weight2, [(2, 0)], half)
    enter(3)
    same = conv_same(first, weight1, [(0, 3)], ins)
    enter(2)
    sides = [conv_next(first, weight1, [last], ins, h) for h in (0, 2)]
    middle(3, same, sides, 1, part1[1], 2)
    same = conv_same(first, weight1, [(0, 2), (1, 3)], ins)
    enter(1)
    middle(2, same, sides, 0, part1[0], 3)
    enter(0)
    sides = [conv_next(first, weight1, [late, early], ins, h) for h in (0, 2)]
    same = conv_same(first, weight1, [(0, 1), (1, 2), (2, 3)], ins)
    middle(1, same, sides, 1, None, 2)
    same = conv_same(first, weight1, [(0, 0), (1, 1), (2, 2)], ins)
    middle(0, same, sides, 0, None, 0)
    sides = [conv_next(second, weight2, [last], outs, h) for h in (0, 2)]
    leave(3, conv_same(second, weight2, [(0, 3)], outs), sides, 1, own3)
    leave(2, conv_same(second, weight2, [(0, 2), (1, 3)], outs), sides, 0, own2)
    same = conv_same(second, weight2, [(0, 1), (1, 2), (2, 3)], outs)
    sides = [conv_next(second, weight2, [late, early], outs, h) for h in (0, 2)]
    leave(1, same, sides, 1, None)
    leave(0, conv_same(second, weight2, [(0, 0), (1, 1), (2, 2)], outs), sides, 0, None)
    for frame in range(frames):
        pltpu.make_async_copy(held.at[frame], out.at[frame], sems.at[frame]).wait()


VMEM = pl.BlockSpec(memory_space=pltpu.VMEM)
OUTSIDE = pl.BlockSpec(memory_space=pltpu.HBM)
MIB = 1024 * 1024


def hbm(array):
    return pltpu.with_memory_space_constraint(array, pltpu.HBM)


def cost(flops):
    return pl.CostEstimate(flops=flops, bytes_accessed=4 * 10**6, transcendentals=0)


def ready(clip):
    frames, _, width, channels = clip.shape
    edge = jax.ShapeDtypeStruct((frames, 2, width, channels), clip.dtype)
    return pl.pallas_call(
        ready_kernel,
        out_shape=[edge, edge],
        in_specs=[VMEM],
        out_specs=[VMEM] * 2,
        compiler_params=pltpu.CompilerParams(vmem_limit_bytes=4 * MIB),
        name="ready",
    )(clip)


def near(place, clip, vectors, weight1, weight2):
    frames, rows, width, channels = clip.shape
    bf16, f32 = jnp.bfloat16, jnp.float32
    outside = [hbm(v.reshape(1, channels)) for v in vectors] + [hbm(weight1), hbm(weight2)]
    return pl.pallas_call(
        functools.partial(near_kernel, place),
        out_shape=[
            jax.ShapeDtypeStruct((frames, (rows // 2 + 1) * width, 2 * channels), f32),
            jax.ShapeDtypeStruct((3, 2, rows + 2, width, channels), bf16),
            jax.ShapeDtypeStruct((6, 1, channels), f32),
            jax.ShapeDtypeStruct(weight1.shape, bf16),
            jax.ShapeDtypeStruct(weight2.shape, bf16),
        ],
        in_specs=[VMEM] + [OUTSIDE] * 8,
        out_specs=[VMEM] * 5,
        scratch_shapes=[
            pltpu.VMEM((3, frames, rows + 4, width, channels), bf16),
            pltpu.VMEM(slot_shape(4, rows + 4, width, channels), f32),
            pltpu.SemaphoreType.DMA((8,)),
        ],
        compiler_params=pltpu.CompilerParams(vmem_limit_bytes=24 * MIB),
        cost_estimate=cost(4 * 10**9),
        name="near",
    )(clip, *outside)


def edge(place, clip, above, below, vectors, weight1, weight2, made):
    frames, rows, width, channels = clip.shape
    bf16, f32 = jnp.bfloat16, jnp.float32
    outside = [hbm(v.reshape(1, channels)) for v in vectors] + [hbm(weight1), hbm(weight2)]
    return pl.pallas_call(
        functools.partial(edge_kernel, place),
        out_shape=[jax.ShapeDtypeStruct(m.shape, m.dtype) for m in made],
        in_specs=[VMEM] * 3 + [OUTSIDE] * 8 + [VMEM] * 5,
        out_specs=[VMEM] * 5,
        input_output_aliases={11 + i: i for i in range(5)},
        scratch_shapes=[
            pltpu.VMEM((3, frames, rows + 4, width, channels), bf16),
            pltpu.VMEM((3, frames, 4, width, channels), bf16),
            pltpu.VMEM(slot_shape(4, rows + 4, width, channels), f32),
            pltpu.SemaphoreType.DMA((8,)),
        ],
        compiler_params=pltpu.CompilerParams(vmem_limit_bytes=24 * MIB),
        cost_estimate=cost(2 * 10**9),
        name="edge",
    )(clip, above, below, *outside, *made)


def far(place, clip, above, below, behind, behind_above, behind_below, part1, own, table, weight1, weight2):
    frames, rows, width, channels = clip.shape
    bf16, f32 = jnp.bfloat16, jnp.float32
    return pl.pallas_call(
        functools.partial(far_kernel, place),
        out_shape=jax.ShapeDtypeStruct(clip.shape, clip.dtype),
        in_specs=[VMEM] * 11,
        out_specs=OUTSIDE,
        scratch_shapes=[
            pltpu.VMEM((3, frames, rows + 4, width, channels), bf16),
            pltpu.VMEM((3, frames, rows + 2, width, channels), bf16),
            pltpu.VMEM(slot_shape(4, rows + 4, width, channels), f32),
            pltpu.VMEM(clip.shape, clip.dtype),
            pltpu.SemaphoreType.DMA((frames,)),
        ],
        compiler_params=pltpu.CompilerParams(vmem_limit_bytes=24 * MIB),
        cost_estimate=cost(4 * 10**9),
        name="far",
    )(clip, above, below, behind, behind_above, behind_below, part1, own, table, weight1, weight2)


def body(
    video,
    norm1_gain,
    norm1_shift,
    conv1_weight,
    conv1_bias,
    norm2_gain,
    norm2_shift,
    conv2_weight,
    conv2_bias,
):
    clip = video[0]
    spans, slabs = lax.axis_size("ta"), lax.axis_size("ha")
    vectors = (norm1_gain, norm1_shift, conv1_bias, norm2_gain, norm2_shift, conv2_bias)

    def place():
        slab = lax.axis_index("ha")
        return lax.axis_index("ta") == 0, slab > 0, slab < slabs - 1

    def at(h, t):
        return h * spans + t

    up = [(h, h + 1) for h in range(slabs - 1)]
    on = [(t, t + 1) for t in range(spans - 1)]

    behind = lax.ppermute(clip, "ta", on)
    top, bottom = ready(clip)
    behind_below = lax.ppermute(top, ("ha", "ta"), [(at(h, t), at(g, n)) for g, h in up for t, n in on])
    made = near(place, clip, vectors, conv1_weight, conv2_weight)
    below = lax.ppermute(top, "ha", [(h, g) for g, h in up])
    above = lax.ppermute(bottom, "ha", up)
    behind_above = lax.ppermute(bottom, ("ha", "ta"), [(at(g, t), at(h, n)) for g, h in up for t, n in on])
    made = edge(place, clip, above, below, vectors, conv1_weight, conv2_weight, made)
    part1, own, table, weight1, weight2 = made
    out = far(
        place, clip, above, below, behind, behind_above, behind_below, part1, own, table, weight1, weight2
    )
    return out[None]


def solution(mesh):
    placed = (P(("grp", "cam"), "ta", "ha", None, None), P(), P(), P(), P(), P(), P(), P(), P())
    return jax.shard_map(
        body,
        mesh=mesh,
        in_specs=placed,
        out_specs=P(("grp", "cam"), "ta", "ha", None, None),
        check_vma=False,
    )
```

```python
import functools

import jax
import jax.numpy as jnp
from jax import lax
from jax.experimental import pallas as pl
from jax.experimental.pallas import tpu as pltpu
from jax.sharding import PartitionSpec as P


EPS = 1e-06
PAD = 8


def activate(values, gain, shift):
    middle = jnp.mean(values, axis=-1, keepdims=True)
    centred = values - middle
    spread = jnp.mean(centred * centred, axis=-1, keepdims=True)
    half = centred * lax.rsqrt(spread + EPS) * gain + shift
    return half + half * jnp.tanh(half)


def put_shifted(ref, frame, row, slots, group, values):
    width = values.shape[0]
    start = row * (width + PAD) + PAD
    slots[group, start : start + width] = values
    ref[0, frame, row] = slots[group, start - 1 : start - 1 + width].astype(ref.dtype)
    ref[1, frame, row] = values.astype(ref.dtype)
    ref[2, frame, row] = slots[group, start + 1 : start + 1 + width].astype(ref.dtype)


def slot_shape(groups, rows, width, channels):
    return groups, rows * (width + PAD) + PAD, channels


def clear_slots(slots, width):
    for group in range(slots.shape[0]):
        for start in range(0, slots.shape[1], width + PAD):
            slots[group, start : start + PAD] = jnp.zeros((PAD, slots.shape[2]), slots.dtype)


def pair_taps(weight_ref, step_t, step_w):
    top, mid, low = (weight_ref[step_t, i, step_w] for i in range(3))
    none = jnp.zeros_like(top)
    upper = jnp.concatenate([jnp.concatenate([top, none], 1), jnp.concatenate([mid, top], 1)], 0)
    lower = jnp.concatenate([jnp.concatenate([low, mid], 1), jnp.concatenate([none, low], 1)], 0)
    return upper, lower


def conv_pairs(maps_ref, weight_ref, taps, pairs):
    total = None
    for step_t, frame in taps:
        for step_w in range(3):
            for skip, rhs in enumerate(pair_taps(weight_ref, step_t, step_w)):
                rows = [2 * (skip + k) for k in range(pairs)]
                left = jnp.concatenate([maps_ref[step_w, frame, r] for r in rows], 0)
                right = jnp.concatenate([maps_ref[step_w, frame, r + 1] for r in rows], 0)
                lhs = jnp.concatenate([left, right], 1)
                part = jnp.dot(lhs, rhs, preferred_element_type=jnp.float32)
                total = part if total is None else total + part
    return total


def pick(total, row, width, channels):
    pair, half = divmod(row, 2)
    return total[pair * width : (pair + 1) * width, half * channels : (half + 1) * channels]


def ready_kernel(video, top, bottom):
    top[...] = video[:, : top.shape[1]]
    bottom[...] = video[:, video.shape[1] - bottom.shape[1] :]


def masked(values, valid):
    return values if valid is None else jnp.where(valid, values, 0.0)


def own_sums(video, vectors, weights_hbm, table, weights, part1, second, first, slots, sems):
    _, rows, width, channels = video.shape
    loads = [pltpu.make_async_copy(v, table.at[i], sems.at[i]) for i, v in enumerate(vectors)]
    loads += [pltpu.make_async_copy(h, w, sems.at[6 + i]) for i, (h, w) in enumerate(zip(weights_hbm, weights))]
    for load in loads:
        load.start()
    clear_slots(slots, width)
    for load in loads[:6]:
        load.wait()
    g1, s1, b1, g2, s2, _ = (table[i] for i in range(6))
    g1, s1, g2, s2 = 0.5 * g1, 0.5 * s1, 0.5 * g2, 0.5 * s2
    half = rows // 2

    def enter(frame):
        for row in range(rows):
            values = activate(video[frame, row].astype(jnp.float32), g1, s1)
            put_shifted(first, frame, row + 2, slots, frame % 2, values)
        for row in (0, 1, rows + 2, rows + 3):
            for step_w in range(3):
                first[step_w, frame, row] = jnp.zeros((width, channels), first.dtype)

    def middle(total, frame, to):
        part1[frame] = total
        for row in range(2, rows):
            values = activate(pick(total, row, width, channels) + b1, g2, s2)
            put_shifted(second, to, row, slots, 2 + to, values)

    enter(0)
    loads[6].wait()
    part1[0] = conv_pairs(first, weights[0], [(2, 0)], half + 1)
    enter(1)
    part1[1] = conv_pairs(first, weights[0], [(1, 0), (2, 1)], half + 1)
    enter(2)
    middle(conv_pairs(first, weights[0], [(0, 0), (1, 1), (2, 2)], half + 1), 2, 0)
    enter(3)
    middle(conv_pairs(first, weights[0], [(0, 1), (1, 2), (2, 3)], half + 1), 3, 1)
    loads[7].wait()


def near_kernel(
    place, video, v0, v1, v2, v3, v4, v5, weight1_hbm, weight2_hbm,
    part1, second, table, weight1, weight2, first, slots, sems,
):
    is_top = jnp.logical_not(place()[1])

    @pl.when(jnp.logical_not(is_top))
    def _():
        own_sums(
            video, (v0, v1, v2, v3, v4, v5), (weight1_hbm, weight2_hbm),
            table, (weight1, weight2), part1, second, first, slots, sems,
        )


def edge_kernel(
    place, video, above, below, v0, v1, v2, v3, v4, v5, weight1_hbm, weight2_hbm, *refs,
):
    part1, second, table, weight1, weight2, first, halo, slots, sems = refs[5:]
    frames, rows, width, channels = video.shape
    _, has_above, has_below = place()

    @pl.when(jnp.logical_not(has_above))
    def _():
        own_sums(
            video, (v0, v1, v2, v3, v4, v5), (weight1_hbm, weight2_hbm),
            table, (weight1, weight2), part1, second, first, slots, sems,
        )

    clear_slots(slots, width)
    g1, s1, b1, g2, s2, _ = (table[i] for i in range(6))
    g1, s1, g2, s2 = 0.5 * g1, 0.5 * s1, 0.5 * g2, 0.5 * s2
    half = rows // 2
    sides = ((above, has_above, 0, 0), (below, has_below, 1, half))
    for frame in range(frames):
        for ref, valid, side, _ in sides:
            for k in range(2):
                values = masked(activate(ref[frame, k].astype(jnp.float32), g1, s1), valid)
                put_shifted(halo, frame, 2 * side + k, slots, frame, values)
    sums = {}
    for _, _, side, pair in sides:
        for step_t in range(3):
            count = frames - 2 + step_t
            total = None
            for step_w in range(3):
                rhs = pair_taps(weight1, step_t, step_w)[side]
                left = jnp.concatenate([halo[step_w, f, 2 * side] for f in range(count)], 0)
                right = jnp.concatenate([halo[step_w, f, 2 * side + 1] for f in range(count)], 0)
                part = jnp.dot(jnp.concatenate([left, right], 1), rhs, preferred_element_type=jnp.float32)
                total = part if total is None else total + part
            for f in range(count):
                to = f + 2 - step_t
                part = total[f * width : (f + 1) * width]
                sums[side, to] = part if (side, to) not in sums else sums[side, to] + part
    for to in range(frames):
        for _, valid, side, pair in sides:
            total = part1[to, pair * width : (pair + 1) * width] + sums[side, to]
            if to < 2:
                part1[to, pair * width : (pair + 1) * width] = total
                continue
            for k in range(2):
                row = 2 * pair + k
                values = activate(pick(total, k, width, channels) + b1, g2, s2)
                values = masked(values, valid if row in (0, rows + 1) else None)
                put_shifted(second, to - 2, row, slots, to - 2, values)


def conv_same(maps_ref, weight_ref, taps, rows):
    total = None
    for step_t, frame in taps:
        for step_w in range(3):
            top, mid, low = (weight_ref[step_t, i, step_w] for i in range(3))
            rhs = jnp.concatenate([jnp.concatenate([mid, top], 1), jnp.concatenate([low, mid], 1)], 0)
            left = jnp.concatenate([maps_ref[step_w, frame, r + 1] for r in rows], 0)
            right = jnp.concatenate([maps_ref[step_w, frame, r + 2] for r in rows], 0)
            part = jnp.dot(jnp.concatenate([left, right], 1), rhs, preferred_element_type=jnp.float32)
            total = part if total is None else total + part
    return total


def conv_next(maps_ref, weight_ref, pairs, rows, step_h):
    total = None
    for frames, steps in pairs:
        for step_w in range(3):
            none = jnp.zeros(weight_ref.shape[3:], weight_ref.dtype)
            blocks = [[none if t is None else weight_ref[t, step_h, step_w] for t in line] for line in steps]
            rhs = jnp.concatenate([jnp.concatenate(line, 1) for line in blocks], 0)
            sides = [jnp.concatenate([maps_ref[step_w, f, r + 3 * (step_h // 2)] for r in rows], 0) for f in frames]
            part = jnp.dot(jnp.concatenate(sides, 1), rhs, preferred_element_type=jnp.float32)
            total = part if total is None else total + part
    return total


def far_kernel(
    place, video, above, below, behind, behind_above, behind_below, part1, own,
    table, weight1, weight2, out, first, second, slots, held, sems,
):
    frames, rows, width, channels = video.shape
    is_start, has_above, has_below = place()
    g1, s1, b1, g2, s2, b2 = (table[i] for i in range(6))
    g1, s1, g2, s2 = 0.5 * g1, 0.5 * s1, 0.5 * g2, 0.5 * s2
    clear_slots(slots, width)

    def enter(frame):
        for row in range(-2, rows + 2):
            at = row + 2 if row < 0 else row - rows if row >= rows else row
            ref, mine = (behind_above, above) if row < 0 else (behind_below, below) if row >= rows else (behind, video)
            values = ref[frame, at]
            if frame >= frames - 2:
                values = jnp.where(is_start, mine[0, at], values)
            values = activate(values.astype(jnp.float32), g1, s1)
            values = masked(values, has_above if row < 0 else has_below if row >= rows else None)
            put_shifted(first, frame, row + 2, slots, frame % 2, values)

    def gather(same, sides, which, row):
        pair, half = divmod(row, 2)
        lines = slice(pair * width, (pair + 1) * width)
        values = same[lines, half * channels : (half + 1) * channels]
        return values + sides[half][lines, which * channels : (which + 1) * channels]

    def middle(to, same, sides, which, more, group):
        for row in range(rows + 2):
            values = gather(same, sides, which, row)
            if more is not None:
                values = values + pick(more, row, width, channels)
            values = activate(values + b1, g2, s2)
            values = masked(values, has_above if row == 0 else has_below if row == rows + 1 else None)
            if to < 2:
                start = row * (width + PAD) + PAD
                values = jnp.where(is_start, slots[3, start : start + width], values)
            put_shifted(second, to, row, slots, group, values)

    def leave(frame, same, sides, which, more):
        for row in range(rows):
            values = gather(same, sides, which, row) + b2
            if more is not None:
                values = values + gather(more, own_sides, which, row)
            held[frame, row] = (video[frame, row].astype(jnp.float32) + values).astype(out.dtype)
        pltpu.make_async_copy(held.at[frame], out.at[frame], sems.at[frame]).start()

    ins, outs = range(0, rows + 2, 2), range(0, rows, 2)
    early, late = (((0, 1), ((0, None), (1, 0))), ((2, 3), ((2, 1), (None, 2))))
    last = ((2, 3), ((0, None), (1, 0)))
    own3 = conv_same(own, weight2, [(1, 0), (2, 1)], outs)
    own2 = conv_same(own, weight2, [(2, 0)], outs)
    own_sides = [conv_next(own, weight2, [((0, 1), ((2, 1), (None, 2)))], outs, h) for h in (0, 2)]
    enter(3)
    same = conv_same(first, weight1, [(0, 3)], ins)
    enter(2)
    sides = [conv_next(first, weight1, [last], ins, h) for h in (0, 2)]
    middle(3, same, sides, 1, part1[1], 2)
    same = conv_same(first, weight1, [(0, 2), (1, 3)], ins)
    enter(1)
    middle(2, same, sides, 0, part1[0], 3)
    enter(0)
    sides = [conv_next(first, weight1, [late, early], ins, h) for h in (0, 2)]
    same = conv_same(first, weight1, [(0, 1), (1, 2), (2, 3)], ins)
    middle(1, same, sides, 1, None, 2)
    same = conv_same(first, weight1, [(0, 0), (1, 1), (2, 2)], ins)
    middle(0, same, sides, 0, None, 0)
    sides = [conv_next(second, weight2, [last], outs, h) for h in (0, 2)]
    leave(3, conv_same(second, weight2, [(0, 3)], outs), sides, 1, own3)
    leave(2, conv_same(second, weight2, [(0, 2), (1, 3)], outs), sides, 0, own2)
    same = conv_same(second, weight2, [(0, 1), (1, 2), (2, 3)], outs)
    sides = [conv_next(second, weight2, [late, early], outs, h) for h in (0, 2)]
    leave(1, same, sides, 1, None)
    leave(0, conv_same(second, weight2, [(0, 0), (1, 1), (2, 2)], outs), sides, 0, None)
    for frame in range(frames):
        pltpu.make_async_copy(held.at[frame], out.at[frame], sems.at[frame]).wait()


VMEM = pl.BlockSpec(memory_space=pltpu.VMEM)
OUTSIDE = pl.BlockSpec(memory_space=pltpu.HBM)
MIB = 1024 * 1024


def hbm(array):
    return pltpu.with_memory_space_constraint(array, pltpu.HBM)


def cost(flops):
    return pl.CostEstimate(flops=flops, bytes_accessed=4 * 10**6, transcendentals=0)


def ready(clip):
    frames, _, width, channels = clip.shape
    edge = jax.ShapeDtypeStruct((frames, 2, width, channels), clip.dtype)
    return pl.pallas_call(
        ready_kernel,
        out_shape=[edge, edge],
        in_specs=[VMEM],
        out_specs=[VMEM] * 2,
        compiler_params=pltpu.CompilerParams(vmem_limit_bytes=4 * MIB),
        name="ready",
    )(clip)


def near(place, clip, vectors, weight1, weight2):
    frames, rows, width, channels = clip.shape
    bf16, f32 = jnp.bfloat16, jnp.float32
    outside = [hbm(v.reshape(1, channels)) for v in vectors] + [hbm(weight1), hbm(weight2)]
    return pl.pallas_call(
        functools.partial(near_kernel, place),
        out_shape=[
            jax.ShapeDtypeStruct((frames, (rows // 2 + 1) * width, 2 * channels), f32),
            jax.ShapeDtypeStruct((3, 2, rows + 2, width, channels), bf16),
            jax.ShapeDtypeStruct((6, 1, channels), f32),
            jax.ShapeDtypeStruct(weight1.shape, bf16),
            jax.ShapeDtypeStruct(weight2.shape, bf16),
        ],
        in_specs=[VMEM] + [OUTSIDE] * 8,
        out_specs=[VMEM] * 5,
        scratch_shapes=[
            pltpu.VMEM((3, frames, rows + 4, width, channels), bf16),
            pltpu.VMEM(slot_shape(4, rows + 4, width, channels), f32),
            pltpu.SemaphoreType.DMA((8,)),
        ],
        compiler_params=pltpu.CompilerParams(vmem_limit_bytes=24 * MIB),
        cost_estimate=cost(4 * 10**9),
        name="near",
    )(clip, *outside)


def edge(place, clip, above, below, vectors, weight1, weight2, made):
    frames, rows, width, channels = clip.shape
    bf16, f32 = jnp.bfloat16, jnp.float32
    outside = [hbm(v.reshape(1, channels)) for v in vectors] + [hbm(weight1), hbm(weight2)]
    return pl.pallas_call(
        functools.partial(edge_kernel, place),
        out_shape=[jax.ShapeDtypeStruct(m.shape, m.dtype) for m in made],
        in_specs=[VMEM] * 3 + [OUTSIDE] * 8 + [VMEM] * 5,
        out_specs=[VMEM] * 5,
        input_output_aliases={11 + i: i for i in range(5)},
        scratch_shapes=[
            pltpu.VMEM((3, frames, rows + 4, width, channels), bf16),
            pltpu.VMEM((3, frames, 4, width, channels), bf16),
            pltpu.VMEM(slot_shape(4, rows + 4, width, channels), f32),
            pltpu.SemaphoreType.DMA((8,)),
        ],
        compiler_params=pltpu.CompilerParams(vmem_limit_bytes=24 * MIB),
        cost_estimate=cost(2 * 10**9),
        name="edge",
    )(clip, above, below, *outside, *made)


def far(place, clip, above, below, behind, behind_above, behind_below, part1, own, table, weight1, weight2):
    frames, rows, width, channels = clip.shape
    bf16, f32 = jnp.bfloat16, jnp.float32
    return pl.pallas_call(
        functools.partial(far_kernel, place),
        out_shape=jax.ShapeDtypeStruct(clip.shape, clip.dtype),
        in_specs=[VMEM] * 11,
        out_specs=OUTSIDE,
        scratch_shapes=[
            pltpu.VMEM((3, frames, rows + 4, width, channels), bf16),
            pltpu.VMEM((3, frames, rows + 2, width, channels), bf16),
            pltpu.VMEM(slot_shape(4, rows + 4, width, channels), f32),
            pltpu.VMEM(clip.shape, clip.dtype),
            pltpu.SemaphoreType.DMA((frames,)),
        ],
        compiler_params=pltpu.CompilerParams(vmem_limit_bytes=24 * MIB),
        cost_estimate=cost(4 * 10**9),
        name="far",
    )(clip, above, below, behind, behind_above, behind_below, part1, own, table, weight1, weight2)


def body(
    video,
    norm1_gain,
    norm1_shift,
    conv1_weight,
    conv1_bias,
    norm2_gain,
    norm2_shift,
    conv2_weight,
    conv2_bias,
):
    clip = video[0]
    spans, slabs = lax.axis_size("ta"), lax.axis_size("ha")
    vectors = (norm1_gain, norm1_shift, conv1_bias, norm2_gain, norm2_shift, conv2_bias)

    def place():
        slab = lax.axis_index("ha")
        return lax.axis_index("ta") == 0, slab > 0, slab < slabs - 1

    def at(h, t):
        return h * spans + t

    up = [(h, h + 1) for h in range(slabs - 1)]
    on = [(t, t + 1) for t in range(spans - 1)]

    behind = lax.ppermute(clip, "ta", on)
    top, bottom = ready(clip)
    behind_below = lax.ppermute(top, ("ha", "ta"), [(at(h, t), at(g, n)) for g, h in up for t, n in on])
    above = lax.ppermute(bottom, "ha", up)
    made = near(place, clip, vectors, conv1_weight, conv2_weight)
    below = lax.ppermute(top, "ha", [(h, g) for g, h in up])
    behind_above = lax.ppermute(bottom, ("ha", "ta"), [(at(g, t), at(h, n)) for g, h in up for t, n in on])
    made = edge(place, clip, above, below, vectors, conv1_weight, conv2_weight, made)
    part1, own, table, weight1, weight2 = made
    out = far(
        place, clip, above, below, behind, behind_above, behind_below, part1, own, table, weight1, weight2
    )
    return out[None]


def solution(mesh):
    placed = (P(("grp", "cam"), "ta", "ha", None, None), P(), P(), P(), P(), P(), P(), P(), P())
    return jax.shard_map(
        body,
        mesh=mesh,
        in_specs=placed,
        out_specs=P(("grp", "cam"), "ta", "ha", None, None),
        check_vma=False,
    )
```

```python
import functools

import jax
import jax.numpy as jnp
from jax import lax
from jax.experimental import pallas as pl
from jax.experimental.pallas import tpu as pltpu
from jax.sharding import PartitionSpec as P


EPS = 1e-06
PAD = 8


def activate(values, gain, shift):
    middle = jnp.mean(values, axis=-1, keepdims=True)
    centred = values - middle
    spread = jnp.mean(centred * centred, axis=-1, keepdims=True)
    half = centred * lax.rsqrt(spread + EPS) * gain + shift
    return half + half * jnp.tanh(half)


def put_shifted(ref, frame, row, slots, group, values):
    width = values.shape[0]
    start = row * (width + PAD) + PAD
    slots[group, start : start + width] = values
    ref[0, frame, row] = slots[group, start - 1 : start - 1 + width].astype(ref.dtype)
    ref[1, frame, row] = values.astype(ref.dtype)
    ref[2, frame, row] = slots[group, start + 1 : start + 1 + width].astype(ref.dtype)


def slot_shape(groups, rows, width, channels):
    return groups, rows * (width + PAD) + PAD, channels


def clear_slots(slots, width):
    for group in range(slots.shape[0]):
        for start in range(0, slots.shape[1], width + PAD):
            slots[group, start : start + PAD] = jnp.zeros((PAD, slots.shape[2]), slots.dtype)


def pair_taps(weight_ref, step_t, step_w):
    top, mid, low = (weight_ref[step_t, i, step_w] for i in range(3))
    none = jnp.zeros_like(top)
    upper = jnp.concatenate([jnp.concatenate([top, none], 1), jnp.concatenate([mid, top], 1)], 0)
    lower = jnp.concatenate([jnp.concatenate([low, mid], 1), jnp.concatenate([none, low], 1)], 0)
    return upper, lower


def conv_pairs(maps_ref, weight_ref, taps, pairs):
    total = None
    for step_t, frame in taps:
        for step_w in range(3):
            for skip, rhs in enumerate(pair_taps(weight_ref, step_t, step_w)):
                rows = [2 * (skip + k) for k in range(pairs)]
                left = jnp.concatenate([maps_ref[step_w, frame, r] for r in rows], 0)
                right = jnp.concatenate([maps_ref[step_w, frame, r + 1] for r in rows], 0)
                lhs = jnp.concatenate([left, right], 1)
                part = jnp.dot(lhs, rhs, preferred_element_type=jnp.float32)
                total = part if total is None else total + part
    return total


def pick(total, row, width, channels):
    pair, half = divmod(row, 2)
    return total[pair * width : (pair + 1) * width, half * channels : (half + 1) * channels]


def ready_kernel(video, top, bottom, sems):
    loads = [
        pltpu.make_async_copy(video.at[:, : top.shape[1]], top, sems.at[0]),
        pltpu.make_async_copy(video.at[:, video.shape[1] - bottom.shape[1] :], bottom, sems.at[1]),
    ]
    for load in loads:
        load.start()
    for load in loads:
        load.wait()


def masked(values, valid):
    return values if valid is None else jnp.where(valid, values, 0.0)


def own_sums(video, vectors, weights_hbm, table, weights, part1, second, first, slots, sems):
    _, rows, width, channels = video.shape
    loads = [pltpu.make_async_copy(v, table.at[i], sems.at[i]) for i, v in enumerate(vectors)]
    loads += [pltpu.make_async_copy(h, w, sems.at[6 + i]) for i, (h, w) in enumerate(zip(weights_hbm, weights))]
    for load in loads:
        load.start()
    clear_slots(slots, width)
    for load in loads[:6]:
        load.wait()
    g1, s1, b1, g2, s2, _ = (table[i] for i in range(6))
    g1, s1, g2, s2 = 0.5 * g1, 0.5 * s1, 0.5 * g2, 0.5 * s2
    half = rows // 2

    def enter(frame):
        for row in range(rows):
            values = activate(video[frame, row].astype(jnp.float32), g1, s1)
            put_shifted(first, frame, row + 2, slots, frame % 2, values)
        for row in (0, 1, rows + 2, rows + 3):
            for step_w in range(3):
                first[step_w, frame, row] = jnp.zeros((width, channels), first.dtype)

    def middle(total, frame, to):
        part1[frame] = total
        for row in range(2, rows):
            values = activate(pick(total, row, width, channels) + b1, g2, s2)
            put_shifted(second, to, row, slots, 2 + to, values)

    enter(0)
    loads[6].wait()
    part1[0] = conv_pairs(first, weights[0], [(2, 0)], half + 1)
    enter(1)
    part1[1] = conv_pairs(first, weights[0], [(1, 0), (2, 1)], half + 1)
    enter(2)
    middle(conv_pairs(first, weights[0], [(0, 0), (1, 1), (2, 2)], half + 1), 2, 0)
    enter(3)
    middle(conv_pairs(first, weights[0], [(0, 1), (1, 2), (2, 3)], half + 1), 3, 1)
    loads[7].wait()


def near_kernel(
    place, video, v0, v1, v2, v3, v4, v5, weight1_hbm, weight2_hbm,
    part1, second, table, weight1, weight2, first, slots, sems,
):
    is_top = jnp.logical_not(place()[1])

    @pl.when(jnp.logical_not(is_top))
    def _():
        own_sums(
            video, (v0, v1, v2, v3, v4, v5), (weight1_hbm, weight2_hbm),
            table, (weight1, weight2), part1, second, first, slots, sems,
        )


def conv_same(maps_ref, weight_ref, taps, rows):
    total = None
    for step_t, frame in taps:
        for step_w in range(3):
            top, mid, low = (weight_ref[step_t, i, step_w] for i in range(3))
            rhs = jnp.concatenate([jnp.concatenate([mid, top], 1), jnp.concatenate([low, mid], 1)], 0)
            left = jnp.concatenate([maps_ref[step_w, frame, r + 1] for r in rows], 0)
            right = jnp.concatenate([maps_ref[step_w, frame, r + 2] for r in rows], 0)
            part = jnp.dot(jnp.concatenate([left, right], 1), rhs, preferred_element_type=jnp.float32)
            total = part if total is None else total + part
    return total


def conv_next(maps_ref, weight_ref, pairs, rows, step_h):
    total = None
    for frames, steps in pairs:
        for step_w in range(3):
            none = jnp.zeros(weight_ref.shape[3:], weight_ref.dtype)
            blocks = [[none if t is None else weight_ref[t, step_h, step_w] for t in line] for line in steps]
            rhs = jnp.concatenate([jnp.concatenate(line, 1) for line in blocks], 0)
            sides = [jnp.concatenate([maps_ref[step_w, f, r + 3 * (step_h // 2)] for r in rows], 0) for f in frames]
            part = jnp.dot(jnp.concatenate(sides, 1), rhs, preferred_element_type=jnp.float32)
            total = part if total is None else total + part
    return total


def gather(same, sides, which, row, width, channels):
    pair, half = divmod(row, 2)
    lines = slice(pair * width, (pair + 1) * width)
    values = same[lines, half * channels : (half + 1) * channels]
    return values + sides[half][lines, which * channels : (which + 1) * channels]


def edge_kernel(
    place, video, above, below, v0, v1, v2, v3, v4, v5, weight1_hbm, weight2_hbm, *refs,
):
    part1, second, table, weight1, weight2, first, halo, slots, sems = refs[5:]
    frames, rows, width, channels = video.shape
    _, has_above, has_below = place()

    @pl.when(jnp.logical_not(has_above))
    def _():
        own_sums(
            video, (v0, v1, v2, v3, v4, v5), (weight1_hbm, weight2_hbm),
            table, (weight1, weight2), part1, second, first, slots, sems,
        )

    clear_slots(slots, width)
    g1, s1, b1, g2, s2, _ = (table[i] for i in range(6))
    g1, s1, g2, s2 = 0.5 * g1, 0.5 * s1, 0.5 * g2, 0.5 * s2
    half = rows // 2
    sides = ((above, has_above, 0, 0), (below, has_below, 1, half))
    for frame in range(frames):
        for ref, valid, side, _ in sides:
            for k in range(2):
                values = masked(activate(ref[frame, k].astype(jnp.float32), g1, s1), valid)
                put_shifted(halo, frame, 2 * side + k, slots, frame, values)
    sums = {}
    for _, _, side, pair in sides:
        for step_t in range(3):
            count = frames - 2 + step_t
            total = None
            for step_w in range(3):
                rhs = pair_taps(weight1, step_t, step_w)[side]
                left = jnp.concatenate([halo[step_w, f, 2 * side] for f in range(count)], 0)
                right = jnp.concatenate([halo[step_w, f, 2 * side + 1] for f in range(count)], 0)
                part = jnp.dot(jnp.concatenate([left, right], 1), rhs, preferred_element_type=jnp.float32)
                total = part if total is None else total + part
            for f in range(count):
                to = f + 2 - step_t
                part = total[f * width : (f + 1) * width]
                sums[side, to] = part if (side, to) not in sums else sums[side, to] + part
    for to in range(frames):
        for _, valid, side, pair in sides:
            total = part1[to, pair * width : (pair + 1) * width] + sums[side, to]
            if to < 2:
                part1[to, pair * width : (pair + 1) * width] = total
                continue
            for k in range(2):
                row = 2 * pair + k
                values = activate(pick(total, k, width, channels) + b1, g2, s2)
                values = masked(values, valid if row in (0, rows + 1) else None)
                put_shifted(second, to - 2, row, slots, to - 2, values)


def far_kernel(
    place, video, above, below, behind, behind_above, behind_below, part1, own,
    table, weight1, weight2, out, first, second, slots, held, sems,
):
    frames, rows, width, channels = video.shape
    is_start, has_above, has_below = place()
    g1, s1, b1, g2, s2, b2 = (table[i] for i in range(6))
    g1, s1, g2, s2 = 0.5 * g1, 0.5 * s1, 0.5 * g2, 0.5 * s2
    ins, outs = range(0, rows + 2, 2), range(0, rows, 2)
    early, late, last = ((0, None), (1, 0)), ((2, 1), (None, 2)), ((0, None), (1, 0))

    def enter(to, sources, frame):
        for row in range(-2, rows + 2):
            at = row + 2 if row < 0 else row - rows if row >= rows else row
            ref = sources[0 if row < 0 else 2 if row >= rows else 1]
            values = activate(ref[frame, at].astype(jnp.float32), g1, s1)
            values = masked(values, has_above if row < 0 else has_below if row >= rows else None)
            put_shifted(first, to, row + 2, slots, to % 2, values)

    def middle(to, same, sides, which, more, group):
        for row in range(rows + 2):
            values = gather(same, sides, which, row, width, channels)
            if more is not None:
                values = values + pick(more, row, width, channels)
            values = activate(values + b1, g2, s2)
            values = masked(values, has_above if row == 0 else has_below if row == rows + 1 else None)
            put_shifted(second, to, row, slots, group, values)

    def leave(frame, same, sides, which, more=None, own_sides=None):
        for row in range(rows):
            values = gather(same, sides, which, row, width, channels) + b2
            if more is not None:
                values = values + gather(more, own_sides, which, row, width, channels)
            held[frame, row] = (video[frame, row].astype(jnp.float32) + values).astype(out.dtype)
        pltpu.make_async_copy(held.at[frame], out.at[frame], sems.at[frame]).start()

    def run(start):
        clear_slots(slots, width)
        a, b, c, d = (3, 3, 3, 3) if start else (0, 1, 2, 3)
        old = (behind_above, behind, behind_below)
        own3 = conv_same(own, weight2, [(1, 0), (2, 1)], outs)
        own2 = conv_same(own, weight2, [(2, 0)], outs)
        own_sides = [conv_next(own, weight2, [((0, 1), late)], outs, h) for h in (0, 2)]
        if start:
            enter(d, (above, video, below), 0)
        else:
            enter(d, old, d)
        same = conv_same(first, weight1, [(0, d)], ins)
        if not start:
            enter(c, old, c)
        sides = [conv_next(first, weight1, [((c, d), last)], ins, h) for h in (0, 2)]
        middle(3, same, sides, 1, part1[1], 2)
        same = conv_same(first, weight1, [(0, c), (1, d)], ins)
        if not start:
            enter(b, old, b)
        middle(2, same, sides, 0, part1[0], 3)
        if not start:
            enter(a, old, a)
            sides = [conv_next(first, weight1, [((c, d), late), ((a, b), early)], ins, h) for h in (0, 2)]
            same = conv_same(first, weight1, [(0, b), (1, c), (2, d)], ins)
            middle(1, same, sides, 1, None, 2)
            same = conv_same(first, weight1, [(0, a), (1, b), (2, c)], ins)
            middle(0, same, sides, 0, None, 0)
        a, b, c, d = (2, 2, 2, 3) if start else (0, 1, 2, 3)
        sides = [conv_next(second, weight2, [((c, d), last)], outs, h) for h in (0, 2)]
        leave(3, conv_same(second, weight2, [(0, d)], outs), sides, 1, own3, own_sides)
        leave(2, conv_same(second, weight2, [(0, c), (1, d)], outs), sides, 0, own2, own_sides)
        same = conv_same(second, weight2, [(0, b), (1, c), (2, d)], outs)
        sides = [conv_next(second, weight2, [((c, d), late), ((a, b), early)], outs, h) for h in (0, 2)]
        leave(1, same, sides, 1)
        leave(0, conv_same(second, weight2, [(0, a), (1, b), (2, c)], outs), sides, 0)
        for frame in range(frames):
            pltpu.make_async_copy(held.at[frame], out.at[frame], sems.at[frame]).wait()

    pl.when(is_start)(functools.partial(run, True))
    pl.when(jnp.logical_not(is_start))(functools.partial(run, False))


VMEM = pl.BlockSpec(memory_space=pltpu.VMEM)
OUTSIDE = pl.BlockSpec(memory_space=pltpu.HBM)
MIB = 1024 * 1024


def hbm(array):
    return pltpu.with_memory_space_constraint(array, pltpu.HBM)


def cost(flops):
    return pl.CostEstimate(flops=flops, bytes_accessed=4 * 10**6, transcendentals=0)


def ready(clip):
    frames, _, width, channels = clip.shape
    edge = jax.ShapeDtypeStruct((frames, 2, width, channels), clip.dtype)
    return pl.pallas_call(
        ready_kernel,
        out_shape=[edge, edge],
        in_specs=[OUTSIDE],
        out_specs=[VMEM] * 2,
        scratch_shapes=[pltpu.SemaphoreType.DMA((2,))],
        compiler_params=pltpu.CompilerParams(vmem_limit_bytes=4 * MIB),
        name="ready",
    )(hbm(clip))


def near(place, clip, vectors, weight1, weight2):
    frames, rows, width, channels = clip.shape
    bf16, f32 = jnp.bfloat16, jnp.float32
    outside = [hbm(v.reshape(1, channels)) for v in vectors] + [hbm(weight1), hbm(weight2)]
    return pl.pallas_call(
        functools.partial(near_kernel, place),
        out_shape=[
            jax.ShapeDtypeStruct((frames, (rows // 2 + 1) * width, 2 * channels), f32),
            jax.ShapeDtypeStruct((3, 2, rows + 2, width, channels), bf16),
            jax.ShapeDtypeStruct((6, 1, channels), f32),
            jax.ShapeDtypeStruct(weight1.shape, bf16),
            jax.ShapeDtypeStruct(weight2.shape, bf16),
        ],
        in_specs=[VMEM] + [OUTSIDE] * 8,
        out_specs=[VMEM] * 5,
        scratch_shapes=[
            pltpu.VMEM((3, frames, rows + 4, width, channels), bf16),
            pltpu.VMEM(slot_shape(4, rows + 4, width, channels), f32),
            pltpu.SemaphoreType.DMA((8,)),
        ],
        compiler_params=pltpu.CompilerParams(vmem_limit_bytes=24 * MIB),
        cost_estimate=cost(4 * 10**9),
        name="near",
    )(clip, *outside)


def edge(place, clip, above, below, vectors, weight1, weight2, made):
    frames, rows, width, channels = clip.shape
    bf16, f32 = jnp.bfloat16, jnp.float32
    outside = [hbm(v.reshape(1, channels)) for v in vectors] + [hbm(weight1), hbm(weight2)]
    return pl.pallas_call(
        functools.partial(edge_kernel, place),
        out_shape=[jax.ShapeDtypeStruct(m.shape, m.dtype) for m in made],
        in_specs=[VMEM] * 3 + [OUTSIDE] * 8 + [VMEM] * 5,
        out_specs=[VMEM] * 5,
        input_output_aliases={11 + i: i for i in range(5)},
        scratch_shapes=[
            pltpu.VMEM((3, frames, rows + 4, width, channels), bf16),
            pltpu.VMEM((3, frames, 4, width, channels), bf16),
            pltpu.VMEM(slot_shape(4, rows + 4, width, channels), f32),
            pltpu.SemaphoreType.DMA((8,)),
        ],
        compiler_params=pltpu.CompilerParams(vmem_limit_bytes=24 * MIB),
        cost_estimate=cost(2 * 10**9),
        name="edge",
    )(clip, above, below, *outside, *made)


def far(place, clip, above, below, behind, behind_above, behind_below, part1, own, table, weight1, weight2):
    frames, rows, width, channels = clip.shape
    bf16, f32 = jnp.bfloat16, jnp.float32
    return pl.pallas_call(
        functools.partial(far_kernel, place),
        out_shape=jax.ShapeDtypeStruct(clip.shape, clip.dtype),
        in_specs=[VMEM] * 11,
        out_specs=OUTSIDE,
        scratch_shapes=[
            pltpu.VMEM((3, frames, rows + 4, width, channels), bf16),
            pltpu.VMEM((3, frames, rows + 2, width, channels), bf16),
            pltpu.VMEM(slot_shape(4, rows + 4, width, channels), f32),
            pltpu.VMEM(clip.shape, clip.dtype),
            pltpu.SemaphoreType.DMA((frames,)),
        ],
        compiler_params=pltpu.CompilerParams(vmem_limit_bytes=24 * MIB),
        cost_estimate=cost(4 * 10**9),
        name="far",
    )(clip, above, below, behind, behind_above, behind_below, part1, own, table, weight1, weight2)


def body(
    video,
    norm1_gain,
    norm1_shift,
    conv1_weight,
    conv1_bias,
    norm2_gain,
    norm2_shift,
    conv2_weight,
    conv2_bias,
):
    clip = video[0]
    spans, slabs = lax.axis_size("ta"), lax.axis_size("ha")
    vectors = (norm1_gain, norm1_shift, conv1_bias, norm2_gain, norm2_shift, conv2_bias)

    def place():
        slab = lax.axis_index("ha")
        return lax.axis_index("ta") == 0, slab > 0, slab < slabs - 1

    def at(h, t):
        return h * spans + t

    up = [(h, h + 1) for h in range(slabs - 1)]
    on = [(t, t + 1) for t in range(spans - 1)]

    behind = lax.ppermute(clip, "ta", on)
    top, bottom = ready(clip)
    behind_below = lax.ppermute(top, ("ha", "ta"), [(at(h, t), at(g, n)) for g, h in up for t, n in on])
    above = lax.ppermute(bottom, "ha", up)
    made = near(place, clip, vectors, conv1_weight, conv2_weight)
    below = lax.ppermute(top, "ha", [(h, g) for g, h in up])
    behind_above = lax.ppermute(bottom, ("ha", "ta"), [(at(g, t), at(h, n)) for g, h in up for t, n in on])
    part1, own, table, weight1, weight2 = edge(
        place, clip, above, below, vectors, conv1_weight, conv2_weight, made
    )
    out = far(
        place, clip, above, below, behind, behind_above, behind_below, part1, own, table, weight1, weight2
    )
    return out[None]


def solution(mesh):
    placed = (P(("grp", "cam"), "ta", "ha", None, None), P(), P(), P(), P(), P(), P(), P(), P())
    return jax.shard_map(
        body,
        mesh=mesh,
        in_specs=placed,
        out_specs=P(("grp", "cam"), "ta", "ha", None, None),
        check_vma=False,
    )
```
